256 devices in a mesh: row: 16 (over x, z_hi, core), col: 16 (over z_lo, y).
Axes of the slice: x: 4, y: 4, z: 8 (z_hi: 2, z_lo: 4; z = z_hi * 4 + z_lo), core: 2. Of those that a mesh axis runs over, the one named last changes fastest.
Arguments:
- rhs_c: float32 [3, 2048, 3, 2048], P(None, 'row', None, 'col'), may hold values from -6 to 6
- rhs_f: float32 [3, 2048, 3, 2048], P(None, 'row', None, 'col'), may hold values from -6 to 6
- pencil_a: bfloat16 [3, 2048, 3, 2048], P(None, 'row', None, 'col'), may hold values from -0.5 to 0.5
- pencil_d: bfloat16 [3, 2048, 3, 2048], P(None, 'row', None, 'col'), may hold values from -0.5 to 0.5
- pencil_b: bfloat16 [3, 2048, 3, 2048], P(None, 'row', None, 'col'), may hold values from -0.5 to 0.5
- pencil_e: bfloat16 [3, 2048, 3, 2048], P(None, 'row', None, 'col'), may hold values from -0.5 to 0.5
- d_inverse: float32 [3, 2048, 128], P(None, 'row'), may hold values from -0.25 to 2.5
- left_vectors: float32 [3, 2048, 128], P(None, 'row'), may hold values from -0.25 to 2.5
- left_inverse: float32 [3, 2048, 128], P(None, 'row'), may hold values from -0.25 to 2.5
- left_eigs: float32 [3, 2048], P(None, 'row'), may hold values from 1 to 3
- e_inverse: float32 [3, 2048, 128], P(None, 'col'), may hold values from -0.25 to 2.5
- right_vectors: float32 [3, 2048, 128], P(None, 'col'), may hold values from -0.25 to 2.5
- right_inverse: float32 [3, 2048, 128], P(None, 'col'), may hold values from -0.25 to 2.5
- right_eigs: float32 [3, 2048], P(None, 'col'), may hold values from -3 to -1
Outputs:
- updated_c: float32 [3, 2048, 3, 2048], P(None, 'row', None, 'col')
- updated_f: float32 [3, 2048, 3, 2048], P(None, 'row', None, 'col')
- solved_r: float32 [3, 2048, 3, 2048], P(None, 'row', None, 'col')
- solved_l: float32 [3, 2048, 3, 2048], P(None, 'row', None, 'col')
The draws below stay inside these ranges and needn't reach their ends.
All inputs are finite; a program needn't handle non-finite values.
Results may differ from the reference program's by a relative error of at most 0.0003.
Values may be sent and summed in bfloat16 or wider, within the bound.
No kernel may reach another device: no remote copies, remote signals or barrier semaphores. Data moves between devices by JAX's collectives and lax.ppermute only.
A program may use at most 64 MiB of HBM per device.

```python
import math
import jax
import jax.numpy as jnp
from jax import lax

TILE = 128
ORDER = 6144
STEPS = 3
RT = 3
CT = 3
N_ROW = 16
N_COL = 16


def dominant(key, lead, height, salt):
    key = jax.random.fold_in(key, salt)
    first, second = jax.random.split(key)
    shape = (lead, height, TILE)
    diagonal = jnp.exp(jax.random.uniform(first, shape, jnp.float32, 0.0, math.log(2.0)))
    spread = jnp.clip(0.4 / math.sqrt(TILE) * jax.random.normal(second, shape, jnp.float32), -0.25, 0.25)
    rows = lax.broadcasted_iota(jnp.int32, shape, 1) % TILE
    cols = lax.broadcasted_iota(jnp.int32, shape, 2)
    return jnp.where(rows == cols, diagonal, spread)


def draw_d_inverse(key, part):
    return dominant(key, RT, N_ROW * TILE, 11)


def draw_left_vectors(key, part):
    return dominant(key, RT, N_ROW * TILE, 12)


def draw_left_inverse(key, part):
    return dominant(key, RT, N_ROW * TILE, 13)


def draw_e_inverse(key, part):
    return dominant(key, CT, N_COL * TILE, 14)


def draw_right_vectors(key, part):
    return dominant(key, CT, N_COL * TILE, 15)


def draw_right_inverse(key, part):
    return dominant(key, CT, N_COL * TILE, 16)


def levels(stream_key, dims, shards, low, top_value):
    def one(dim, blocks):
        steps = jax.random.uniform(jax.random.fold_in(jax.random.fold_in(stream_key, 6), dim), (blocks,), jnp.float32, low / len(shards), top_value / len(shards))
        return jnp.repeat(jnp.exp(steps), dims[dim] // blocks).reshape((-1,) + (1,) * (len(dims) - dim - 1))

    factor_of = one(*shards[0])
    for cut in shards[1:]:
        factor_of = factor_of * one(*cut)
    return factor_of


def scatter_about(key, extent, width, limit, cuts=(), kind=jnp.bfloat16):
    entries = width * jax.random.normal(key, extent, jnp.float32)
    if cuts:
        entries = entries * levels(key, extent, cuts, -0.22, 0.18)
    return jnp.clip(entries, -limit, limit).astype(kind)


def setup_inputs(seed: int = 0) -> dict:
    seeds = jax.random.split(jax.random.key(seed), 15)
    return {
        "rhs_c": scatter_about(seeds[0], (RT, N_ROW * TILE, CT, N_COL * TILE), 1.0, 6.0, ((1, 16), (3, 16)), jnp.float32),
        "rhs_f": scatter_about(seeds[1], (RT, N_ROW * TILE, CT, N_COL * TILE), 1.0, 6.0, ((1, 16), (3, 16)), jnp.float32),
        "pencil_a": scatter_about(seeds[2], (RT, N_ROW * TILE, CT, N_COL * TILE), TILE ** -0.5, 0.5, ((1, 16), (3, 16))),
        "pencil_d": scatter_about(seeds[3], (RT, N_ROW * TILE, CT, N_COL * TILE), TILE ** -0.5, 0.5, ((1, 16), (3, 16))),
        "pencil_b": scatter_about(seeds[4], (RT, N_ROW * TILE, CT, N_COL * TILE), TILE ** -0.5, 0.5, ((1, 16), (3, 16))),
        "pencil_e": scatter_about(seeds[5], (RT, N_ROW * TILE, CT, N_COL * TILE), TILE ** -0.5, 0.5, ((1, 16), (3, 16))),
        "d_inverse": draw_d_inverse(jax.random.fold_in(seeds[14], 71), 0),
        "left_vectors": draw_left_vectors(jax.random.fold_in(seeds[14], 71), 0),
        "left_inverse": draw_left_inverse(jax.random.fold_in(seeds[14], 71), 0),
        "left_eigs": jnp.clip(jnp.exp(math.log(3.0) - 1.0986123 * jax.random.uniform(seeds[9], (RT, N_ROW * TILE), jnp.float32) ** levels(seeds[9], (RT, N_ROW * TILE), ((1, 16),), -0.2, 0.2)), 1.0, 3.0),
        "e_inverse": draw_e_inverse(jax.random.fold_in(seeds[14], 71), 0),
        "right_vectors": draw_right_vectors(jax.random.fold_in(seeds[14], 71), 0),
        "right_inverse": draw_right_inverse(jax.random.fold_in(seeds[14], 71), 0),
        "right_eigs": jnp.clip(-3.0 + 2.0 * jax.random.uniform(seeds[13], (CT, N_COL * TILE), jnp.float32) ** levels(seeds[13], (CT, N_COL * TILE), ((1, 16),), -0.2, 0.2), -3.0, -1.0),
    }


def product(left, right):
    return jnp.einsum("bij,bjk->bik", left, right, precision=lax.Precision.HIGHEST)


def solve_tiles(a_diag, e_diag, resid_c, resid_f, inv_d, vec_left, back_left, eig_left, inv_e, vec_right, back_right, eig_right):
    coupled = product(a_diag, inv_d)
    merged = product(resid_c - product(coupled, resid_f), inv_e)
    spectral = product(product(back_left, merged), vec_right)
    spectral = spectral / (eig_left[:, :, None] - eig_right[:, None, :])
    new_l = product(product(vec_left, spectral), back_right)
    new_r = product(inv_d, resid_f + product(new_l, e_diag))
    return new_r, new_l


def reference(rhs_c, rhs_f, pencil_a, pencil_d, pencil_b, pencil_e, d_inverse, left_vectors, left_inverse, left_eigs, e_inverse, right_vectors, right_inverse, right_eigs):
    blocks = ORDER // TILE
    highest = lax.Precision.HIGHEST

    def grid(field):
        return field.astype(jnp.float32).reshape(blocks, TILE, blocks, TILE)

    current_c = grid(rhs_c)
    current_f = grid(rhs_f)
    tiles_a = grid(pencil_a)
    tiles_d = grid(pencil_d)
    tiles_b = grid(pencil_b)
    tiles_e = grid(pencil_e)
    inv_d = d_inverse.reshape(blocks, TILE, TILE)
    vec_left = left_vectors.reshape(blocks, TILE, TILE)
    back_left = left_inverse.reshape(blocks, TILE, TILE)
    eig_left = left_eigs.reshape(blocks, TILE)
    inv_e = e_inverse.reshape(blocks, TILE, TILE)
    vec_right = right_vectors.reshape(blocks, TILE, TILE)
    back_right = right_inverse.reshape(blocks, TILE, TILE)
    eig_right = right_eigs.reshape(blocks, TILE)
    out_r = jnp.zeros_like(current_c)
    out_l = jnp.zeros_like(current_c)
    count = jnp.arange(blocks, dtype=jnp.int32)
    for step in range(STEPS):
        offset = 1 - step
        front_rows = count + offset
        col_valid = (front_rows >= 0) & (front_rows < blocks)
        rows_clip = jnp.clip(front_rows, 0, blocks - 1).astype(jnp.int32)
        front_cols = count - offset
        row_valid = (front_cols >= 0) & (front_cols < blocks)
        cols_clip = jnp.clip(front_cols, 0, blocks - 1).astype(jnp.int32)
        resid_c = current_c[rows_clip, :, count, :]
        resid_f = current_f[rows_clip, :, count, :]
        a_diag = tiles_a[rows_clip, :, rows_clip, :]
        e_diag = tiles_e[count, :, count, :]
        new_r, new_l = solve_tiles(a_diag, e_diag, resid_c, resid_f, inv_d[rows_clip], vec_left[rows_clip], back_left[rows_clip], eig_left[rows_clip], inv_e, vec_right, back_right, eig_right)
        new_r = jnp.where(col_valid[:, None, None], new_r, 0.0)
        new_l = jnp.where(col_valid[:, None, None], new_l, 0.0)
        panel_a = tiles_a[:, :, rows_clip, :]
        panel_d = tiles_d[:, :, rows_clip, :]
        mask_a = (count[:, None] < front_rows[None, :]) & col_valid[None, :]
        term_c = jnp.einsum("kpjq,jqs->kpjs", panel_a, new_r, precision=highest)
        term_f = jnp.einsum("kpjq,jqs->kpjs", panel_d, new_r, precision=highest)
        row_l = jnp.where(row_valid[:, None, None], new_l[cols_clip], 0.0)
        panel_b = tiles_b[cols_clip]
        panel_e = tiles_e[cols_clip]
        mask_b = (count[None, :] > front_cols[:, None]) & row_valid[:, None]
        gain_c = jnp.einsum("ipq,iqls->ipls", row_l, panel_b, precision=highest)
        gain_f = jnp.einsum("ipq,iqls->ipls", row_l, panel_e, precision=highest)
        wide_a = mask_a[:, None, :, None]
        wide_b = mask_b[:, None, :, None]
        current_c = current_c - jnp.where(wide_a, term_c, 0.0) + jnp.where(wide_b, gain_c, 0.0)
        current_f = current_f - jnp.where(wide_a, term_f, 0.0) + jnp.where(wide_b, gain_f, 0.0)
        out_r = out_r.at[rows_clip, :, count, :].add(new_r)
        out_l = out_l.at[rows_clip, :, count, :].add(new_l)
    shape = (RT, N_ROW * TILE, CT, N_COL * TILE)
    return current_c.reshape(shape), current_f.reshape(shape), out_r.reshape(shape), out_l.reshape(shape)
```

```python
import functools

import jax
import jax.numpy as jnp
import numpy as np
from jax import lax
from jax.experimental import pallas as pl
from jax.experimental.pallas import tpu as pltpu
from jax.sharding import PartitionSpec as P


TILE = 128
AXES = ("row", "col")

UPPER = ((0, 0), (0, 1), (0, 2), (1, 1), (1, 2), (2, 2))
SIDE = 16


def split(value):
    high = value.astype(jnp.bfloat16)
    low = (value - high.astype(jnp.float32)).astype(jnp.bfloat16)
    return high, low


def dot(left, right):
    return jnp.dot(left, right, preferred_element_type=jnp.float32)


def mul(left, right):
    lh, ll = split(left)
    rh, rl = split(right)
    return dot(lh, rh) + (dot(lh, rl) + dot(ll, rh))


def mul_bl(left, right):
    rh, rl = split(right)
    return dot(left, rh) + dot(left, rl)


def mul_br(left, right):
    lh, ll = split(left)
    return dot(lh, right) + dot(ll, right)


def row_of(ref, index):
    return ref[pl.ds(index, 1), :]


def finish(b, a, valid, cc, ff, ux, g, ve, du, dinv, u, uinv, vinv, x, y, out_r, out_l):
    m = mul(uinv, cc) - mul(ux, ff)
    w = mul(m, g)
    w = w / (x.reshape(TILE, 1) - y)
    new_l = mul(u, mul(w, vinv))
    new_r = mul(dinv, ff) + mul(du, mul(w, ve))

    @pl.when(valid)
    def _():
        out_r[b] = new_r
        out_l[a] = new_l


def each_slot(scal, fn):
    shift = scal[1]
    for b in range(3):
        row = b + shift
        valid = (row >= 0) & (row <= 2)
        fn(b, jnp.clip(row, 0, 2), valid)


def near_kernel(scal, pa, pd, pb, pe, near_ad, near_be, a_own, e_own):
    row, col = (scal[2], scal[3])
    ahead = lax.rem(col - row + SIDE, SIDE)
    up = jnp.where(row + ahead >= SIDE, 1, 0)
    back = jnp.where(col < ahead, 1, 0)
    for i in range(3):
        right = jnp.minimum(i + up, 2)
        above = jnp.maximum(i - back, 0)
        near_ad[0, i] = pa[i, right]
        near_ad[1, i] = pd[i, right]
        near_be[0, i] = pb[above, i]
        near_be[1, i] = pe[above, i]
        a_own[i] = pa[i, i]
        e_own[i] = pe[i, i]


def upper_kernel(scal, pa, pd, pb, pe, upper_ad, upper_be):
    for at, (a, b) in enumerate(UPPER):
        upper_ad[0, at] = pa[a, b]
        upper_ad[1, at] = pd[a, b]
        upper_be[0, at] = pb[a, b]
        upper_be[1, at] = pe[a, b]


def first_kernel(
    scal, cc, ff, a_own, e_own, col_m, col_p, row_p, row_m, dinv, u, uinv, x, einv, v, vinv, y,
    ux_o, g_o, ve_o, du_o, out_r, out_l,
):
    role = scal[0]
    out_r[...] = jnp.zeros_like(out_r)
    out_l[...] = jnp.zeros_like(out_l)

    @pl.when(role < 3)
    def _():
        def prepare(b, a, valid):
            a_diag = jnp.where(role == 0, col_m[0, a], jnp.where(role == 1, a_own[a], col_p[a]))
            e_diag = jnp.where(role == 0, row_p[1, b], jnp.where(role == 1, e_own[b], row_m[b]))
            coupled = mul_bl(a_diag, dinv[a])
            ux_o[b] = mul(uinv[a], coupled)
            g_o[b] = mul(einv[b], v[b])
            ve_o[b] = mul_br(vinv[b], e_diag)
            du_o[b] = mul(dinv[a], u[a])

        each_slot(scal, prepare)

    @pl.when(role == 0)
    def _():
        def solve(b, a, valid):
            finish(
                b, a, valid, cc[a, b], ff[a, b], ux_o[b], g_o[b], ve_o[b], du_o[b],
                dinv[a], u[a], uinv[a], vinv[b], row_of(x, a), row_of(y, b), out_r, out_l,
            )

        each_slot(scal, solve)


def next_kernel(
    step, scal, cc, ff, pa, pd, pb, pe, col_m, row_p, r_old, l_old,
    dinv, u, uinv, x, vinv, y, ux, g, ve, du, out_r, out_l,
):
    role = scal[0]
    out_r[...] = jnp.zeros_like(out_r)
    out_l[...] = jnp.zeros_like(out_l)
    if step == 1:
        r_far, l_far = (r_old, l_old)
        new_r, new_l = (out_r.at[1], out_l.at[1])
    else:
        r_far, l_far, r_near, l_near = (r_old.at[0], l_old.at[0], r_old.at[1], l_old.at[1])
        new_r, new_l = (out_r, out_l)

    @pl.when(role == step)
    def _():
        if step == 1:
            out_r[0] = r_far[...]
            out_l[0] = l_far[...]

        def solve(b, a, valid):
            c_now = cc[a, b] - mul_bl(col_m[0, a], r_far[b]) + mul_br(l_far[a], row_p[0, b])
            f_now = ff[a, b] - mul_bl(col_m[1, a], r_far[b]) + mul_br(l_far[a], row_p[1, b])
            if step == 2:
                c_now += mul_br(l_near[a], pb[a, b]) - mul_bl(pa[a, b], r_near[b])
                f_now += mul_br(l_near[a], pe[a, b]) - mul_bl(pd[a, b], r_near[b])
            finish(
                b, a, valid, c_now, f_now, ux[b], g[b], ve[b], du[b],
                dinv[a], u[a], uinv[a], vinv[b], row_of(x, a), row_of(y, b), new_r, new_l,
            )

        each_slot(scal, solve)


def last_kernel(
    scal, cc, ff, pa, pd, pb, pe, ad_next, ad_prev, be_prev, be_next, fr_old, fl_old, fr, fl,
    r0, l0, r1, l1, r2, l2, c_out, f_out, r_out, l_out,
):
    role, row, col = (scal[0], scal[2], scal[3])
    diff = col - row
    c_out[...] = cc[...]
    f_out[...] = ff[...]
    r_out[...] = jnp.zeros_like(r_out)
    l_out[...] = jnp.zeros_like(l_out)
    for at, (a, b) in enumerate(UPPER):
        nxt = at + jnp.where(col == SIDE - 1, 1, 0) if b < 2 else at
        prv = at - jnp.where(col == 0, 1, 0) if b > a else at
        above = at - jnp.where(row == 0, 2 if a == 1 else 1, 0) if a > 0 else at
        below = at + jnp.where(row == SIDE - 1, 2 if a == 0 else 1, 0) if b > a else at
        tiles_c = (ad_next[0, nxt], pa[a, b], ad_prev[0, prv])
        tiles_f = (ad_next[1, nxt], pd[a, b], ad_prev[1, prv])
        lines_c = (be_prev[0, above], pb[a, b], be_next[0, below])
        lines_f = (be_prev[1, above], pe[a, b], be_next[1, below])
        sum_c = cc[a, b]
        sum_f = ff[a, b]
        for s in range(3):
            on = SIDE * (b - a) + diff >= s
            rh, rl = split(jnp.where(on, fr[b] if s == 2 else fr_old[s, b], 0.0))
            lh, ll = split(jnp.where(on, fl[a] if s == 2 else fl_old[s, a], 0.0))
            sum_c += (dot(lh, lines_c[s]) + dot(ll, lines_c[s])) - (dot(tiles_c[s], rh) + dot(tiles_c[s], rl))
            sum_f += (dot(lh, lines_f[s]) + dot(ll, lines_f[s])) - (dot(tiles_f[s], rh) + dot(tiles_f[s], rl))
        c_out[a, b] = sum_c
        f_out[a, b] = sum_f

    @pl.when(role < 3)
    def _():
        def place(b, a, valid):
            @pl.when(valid)
            def _():
                r_out[a, b] = r0[b] + r1[1, b] + r2[b]
                l_out[a, b] = l0[a] + l1[1, a] + l2[a]

        each_slot(scal, place)


def halves(*shape):
    return jax.ShapeDtypeStruct((*shape, TILE, TILE), jnp.bfloat16)


SMEM = pl.BlockSpec(memory_space=pltpu.SMEM)
VMEM = pl.BlockSpec(memory_space=pltpu.VMEM)
THREE = jax.ShapeDtypeStruct((3, TILE, TILE), jnp.float32)
PAIR = jax.ShapeDtypeStruct((2, 3, TILE, TILE), jnp.float32)
NINE = jax.ShapeDtypeStruct((3, 3, TILE, TILE), jnp.float32)


def call(kernel, outs, flops, *args):
    return pl.pallas_call(
        kernel,
        out_shape=outs,
        in_specs=[SMEM] + [VMEM] * (len(args) - 1),
        out_specs=[VMEM] * len(outs),
        cost_estimate=pl.CostEstimate(flops=flops, bytes_accessed=4_000_000, transcendentals=0),
    )(*args)


def device(row, col):
    return (row % SIDE) * SIDE + col % SIDE


def send(value, pairs):
    return lax.ppermute(value, AXES, [(device(*s), device(*t)) for s, t in pairs])


class Tree:
    def __init__(self, value, roots, me):
        self.value, self.have, self.me, self.came, self.moves = (value, list(roots), me, [], ())

    def start(self, moves):
        self.moves = moves
        self.came = [send(self.value, [(s, move(*s)) for s in self.have]) for move in moves]

    def finish(self):
        mask = np.zeros(SIDE * SIDE, bool)
        for s in self.have:
            mask[device(*s)] = True
        own = jnp.asarray(mask)[self.me]
        self.value = jnp.where(own, self.value, functools.reduce(jnp.add, self.came))
        self.have += [move(*s) for move in self.moves for s in self.have]

    def after(self, other):
        self.value, _ = lax.optimization_barrier((self.value, other))


def flip_row(bits):
    return lambda row, col: (row ^ bits, col)


def turn_row(step):
    return lambda row, col: ((row + step) % SIDE, col)


def turn_col(step):
    return lambda row, col: (row, (col + step) % SIDE)


def turn_low(step):
    return lambda row, col: (row, (col & ~3) | ((col + step) & 3))


ROW_LEVELS = ((flip_row(2),), (turn_row(4), turn_row(8), turn_row(12)), (flip_row(1),))
COL_LEVELS = ((turn_col(4), turn_col(8), turn_col(12)), (turn_low(1), turn_low(2), turn_low(3)))


def program(
    rhs_c, rhs_f, pencil_a, pencil_d, pencil_b, pencil_e, d_inverse, left_vectors, left_inverse,
    left_eigs, e_inverse, right_vectors, right_inverse, right_eigs,
):
    row = lax.axis_index("row").astype(jnp.int32)
    col = lax.axis_index("col").astype(jnp.int32)
    me = row * SIDE + col
    cc, ff, pa, pd, pb, pe = [
        v.transpose(0, 2, 1, 3) for v in (rhs_c, rhs_f, pencil_a, pencil_d, pencil_b, pencil_e)
    ]
    ahead = (col - row) % SIDE
    role = jnp.where(ahead == SIDE - 1, 0, jnp.where(ahead < 2, ahead + 1, 3))
    shift = jnp.where((role == 0) & (col == SIDE - 1), 1, jnp.where((role == 2) & (col == 0), -1, 0))
    scal = jnp.stack([role, shift, row, col])
    ring = range(SIDE)
    left = (d_inverse, left_vectors, left_inverse, left_eigs)

    near_ad, near_be, a_own, e_own = call(
        near_kernel, [halves(2, 3), halves(2, 3), halves(3), halves(3)], 1_000_000, scal, pa, pd, pb, pe
    )
    col_m = send(near_ad, [((r, r + k), (r, r + k - 1)) for r in ring for k in range(3)])
    row_p = send(near_be, [((r, r + k), (r + 1, r + k)) for r in ring for k in range(3)])
    col_p = send(a_own, [((r, r), (r, r + 1)) for r in ring])
    row_m = send(e_own, [((r, r), (r - 1, r)) for r in ring])

    upper_ad, upper_be = call(
        upper_kernel, [halves(2, 6), halves(2, 6)], 20_000_000, scal, pa, pd, pb, pe
    )
    up = [(i, (i + 1) % SIDE) for i in ring]
    down = [(j, i) for i, j in up]

    ux, g, ve, du, r0, l0 = call(
        first_kernel, [THREE] * 6, 400_000_000,
        scal, cc, ff, a_own, e_own, col_m, col_p, row_p, row_m, *left,
        e_inverse, right_vectors, right_inverse, right_eigs,
    )
    ready = (*left, right_inverse, right_eigs, ux, g, ve, du)
    upper_ad, upper_be, r0, l0 = lax.optimization_barrier((upper_ad, upper_be, r0, l0))
    r0_one = send(r0, [((c + 1, c), (c, c)) for c in ring])
    l0_one = send(l0, [((r, r - 1), (r, r)) for r in ring])
    be_prev = lax.ppermute(upper_be, "row", up)
    be_next = lax.ppermute(upper_be, "row", down)
    ad_next = lax.ppermute(upper_ad, "col", down)
    ad_prev = lax.ppermute(upper_ad, "col", up)
    tiles = (scal, cc, ff, pa, pd, pb, pe, col_m, row_p)
    r1, l1 = call(
        functools.partial(next_kernel, 1), [PAIR] * 2, 400_000_000,
        *tiles, r0_one, l0_one, *ready,
    )
    r_old = send(r1, [((c, c), (c - 1, c)) for c in ring])
    l_old = send(l1, [((r, r), (r, r + 1)) for r in ring])
    r2, l2 = call(
        functools.partial(next_kernel, 2), [THREE] * 2, 400_000_000,
        *tiles, r_old, l_old, *ready,
    )

    early_r = Tree(r1, [(c, c) for c in ring], me)
    early_l = Tree(l1, [(r, r) for r in ring], me)
    late_r = Tree(r2, [((c - 1) % SIDE, c) for c in ring], me)
    late_l = Tree(l2, [(r, (r + 1) % SIDE) for r in ring], me)
    early_r.start(ROW_LEVELS[0])
    early_l.start(COL_LEVELS[0])
    late_r.start(ROW_LEVELS[0])
    late_l.start(COL_LEVELS[0])
    early_r.finish()
    early_l.finish()
    early_r.after(r2)
    early_l.after(r2)
    early_r.start(ROW_LEVELS[1])
    early_l.start(COL_LEVELS[1])
    late_r.finish()
    late_l.finish()
    late_r.start(ROW_LEVELS[1])
    late_l.start(COL_LEVELS[1])
    early_r.finish()
    early_l.finish()
    early_r.start(ROW_LEVELS[2])
    late_r.finish()
    late_l.finish()
    late_r.start(ROW_LEVELS[2])
    early_r.finish()
    late_r.finish()

    outs = call(
        last_kernel, [NINE] * 4, 1_500_000_000,
        scal, cc, ff, pa, pd, pb, pe, ad_next, ad_prev, be_prev, be_next,
        early_r.value, early_l.value, late_r.value, late_l.value, r0, l0, r1, l1, r2, l2,
    )
    return tuple(v.transpose(0, 2, 1, 3) for v in outs)


def solution(mesh):
    tile = P(None, "row", None, "col")
    lines = (P(None, "row", None),) * 3 + (P(None, "row"),)
    cols = (P(None, "col", None),) * 3 + (P(None, "col"),)
    return jax.shard_map(
        program, mesh=mesh, in_specs=(tile,) * 6 + lines + cols, out_specs=(tile,) * 4, check_vma=False
    )
```

```python
import functools

import jax
import jax.numpy as jnp
from jax import lax
from jax.experimental import pallas as pl
from jax.experimental.pallas import tpu as pltpu
from jax.sharding import PartitionSpec as P


TILE = 128
AXES = ("row", "col")

UPPER = ((0, 0), (0, 1), (0, 2), (1, 1), (1, 2), (2, 2))
SIDE = 16


def split(value):
    high = value.astype(jnp.bfloat16)
    low = (value - high.astype(jnp.float32)).astype(jnp.bfloat16)
    return high, low


def dot(left, right):
    return jnp.dot(left, right, preferred_element_type=jnp.float32)


def mul(left, right):
    lh, ll = split(left)
    rh, rl = split(right)
    return dot(lh, rh) + (dot(lh, rl) + dot(ll, rh))


def mul_bl(left, right):
    rh, rl = split(right)
    return dot(left, rh) + dot(left, rl)


def mul_br(left, right):
    lh, ll = split(left)
    return dot(lh, right) + dot(ll, right)


def row_of(ref, index):
    return ref[pl.ds(index, 1), :]


def finish(slots, out_r, out_l):
    m = [mul(t["uinv"], t["c"]) - mul(t["ux"], t["f"]) for t in slots]
    w = [mul(one, t["g"]) for one, t in zip(m, slots)]
    w = [one / (t["x"].reshape(TILE, 1) - t["y"]) for one, t in zip(w, slots)]
    to_l = [mul(one, t["vinv"]) for one, t in zip(w, slots)]
    to_r = [mul(one, t["ve"]) for one, t in zip(w, slots)]
    new_l = [mul(t["u"], one) for one, t in zip(to_l, slots)]
    new_r = [mul(t["dinv"], t["f"]) + mul(t["du"], one) for one, t in zip(to_r, slots)]
    for t, this_r, this_l in zip(slots, new_r, new_l):

        @pl.when(t["valid"])
        def _(t=t, this_r=this_r, this_l=this_l):
            out_r[t["b"]] = this_r
            out_l[t["a"]] = this_l


def fetch(scal, sources, buffers, sem):
    shift = scal[1]
    coming = []
    for b in range(3):
        row = jnp.clip(b + shift, 0, 2)
        coming.append([
            pltpu.make_async_copy(src.at[row, b], buf.at[b], sem.at[n, b])
            for n, (src, buf) in enumerate(zip(sources, buffers))
        ])
        for one in coming[-1]:
            one.start()
    return coming


def slots_of(scal):
    rows = [b + scal[1] for b in range(3)]
    return [(b, jnp.clip(row, 0, 2), (row >= 0) & (row <= 2)) for b, row in enumerate(rows)]


def own_kernel(scal, pa, pd, pb, pe, a_own, e_own, near_ad, near_be):
    row, col = (scal[2], scal[3])
    ahead = lax.rem(col - row + SIDE, SIDE)
    up = jnp.where(row + ahead >= SIDE, 1, 0)
    back = jnp.where(col < ahead, 1, 0)
    for i in range(3):
        a_own[i] = pa[i, i]
        e_own[i] = pe[i, i]
        right = jnp.minimum(i + up, 2)
        above = jnp.maximum(i - back, 0)
        near_ad[0, i] = pa[i, right]
        near_ad[1, i] = pd[i, right]
        near_be[0, i] = pb[above, i]
        near_be[1, i] = pe[above, i]


def upper_kernel(scal, pa, pd, pb, pe, upper_ad, upper_be):
    for at, (a, b) in enumerate(UPPER):
        upper_ad[0, at] = pa[a, b]
        upper_ad[1, at] = pd[a, b]
        upper_be[0, at] = pb[a, b]
        upper_be[1, at] = pe[a, b]


def prepare(tiles, outs):
    coupled = [mul_bl(a, dinv) for a, _, dinv, *_ in tiles]
    ux = [mul(t[4], one) for one, t in zip(coupled, tiles)]
    g = [mul(t[5], t[6]) for t in tiles]
    ve = [mul_br(t[7], t[1]) for t in tiles]
    du = [mul(t[2], t[3]) for t in tiles]
    for out, values in zip(outs, (ux, g, ve, du)):
        for b in range(3):
            out[b] = values[b]
    return ux, g, ve, du


def first_kernel(
    scal, cc, ff, a_own, e_own, a_came, e_came, dinv, u, uinv, x, einv, v, vinv, y,
    ux_o, g_o, ve_o, du_o, out_r, out_l, c_buf, f_buf, sem,
):
    role = scal[0]
    out_r[...] = jnp.zeros_like(out_r)
    out_l[...] = jnp.zeros_like(out_l)
    slots = slots_of(scal)

    @pl.when(role == 1)
    def _():
        tiles = [(a_own[a], e_own[b], dinv[a], u[a], uinv[a], einv[b], v[b], vinv[b]) for b, a, _ in slots]
        prepare(tiles, (ux_o, g_o, ve_o, du_o))

    @pl.when(role == 0)
    def _():
        coming = fetch(scal, (cc, ff), (c_buf, f_buf), sem)
        tiles = [(a_came[a], e_came[b], dinv[a], u[a], uinv[a], einv[b], v[b], vinv[b]) for b, a, _ in slots]
        ux, g, ve, du = prepare(tiles, ())
        for group in coming:
            for one in group:
                one.wait()
        finish(
            [
                dict(
                    b=b, a=a, valid=valid, c=c_buf[b], f=f_buf[b], ux=ux[b], g=g[b], ve=ve[b], du=du[b],
                    dinv=dinv[a], u=u[a], uinv=uinv[a], vinv=vinv[b], x=row_of(x, a), y=row_of(y, b),
                )
                for b, a, valid in slots
            ],
            out_r, out_l,
        )


def ready_kernel(scal, a_prev, e_next, dinv, u, uinv, einv, v, vinv, ux_o, g_o, ve_o, du_o):
    slots = slots_of(scal)

    @pl.when(scal[0] == 2)
    def _():
        tiles = [(a_prev[a], e_next[b], dinv[a], u[a], uinv[a], einv[b], v[b], vinv[b]) for b, a, _ in slots]
        prepare(tiles, (ux_o, g_o, ve_o, du_o))


def next_kernel(
    step, scal, cc, ff, pa, pd, pb, pe, ad_near, be_near, r_old, l_old,
    dinv, u, uinv, x, vinv, y, ux, g, ve, du, out_r, out_l, *bufs,
):
    role = scal[0]
    out_r[...] = jnp.zeros_like(out_r)
    out_l[...] = jnp.zeros_like(out_l)
    if step == 1:
        r_far, l_far = (r_old, l_old)
        new_r, new_l = (out_r.at[1], out_l.at[1])
    else:
        r_far, l_far, r_near, l_near = (r_old.at[0], l_old.at[0], r_old.at[1], l_old.at[1])
        new_r, new_l = (out_r, out_l)

    *bufs, sem = bufs

    @pl.when(role == step)
    def _():
        coming = fetch(scal, (cc, ff, pa, pd, pb, pe)[: len(bufs)], bufs, sem)
        if step == 1:
            out_r[0] = r_far[...]
            out_l[0] = l_far[...]

        for group in coming:
            for one in group:
                one.wait()
        ready = []
        for b, a, valid in slots_of(scal):
            c_now = bufs[0][b] - mul_bl(ad_near[0, a], r_far[b]) + mul_br(l_far[a], be_near[0, b])
            f_now = bufs[1][b] - mul_bl(ad_near[1, a], r_far[b]) + mul_br(l_far[a], be_near[1, b])
            if step == 2:
                c_now += mul_br(l_near[a], bufs[4][b]) - mul_bl(bufs[2][b], r_near[b])
                f_now += mul_br(l_near[a], bufs[5][b]) - mul_bl(bufs[3][b], r_near[b])
            ready.append(
                dict(
                    b=b, a=a, valid=valid, c=c_now, f=f_now, ux=ux[b], g=g[b], ve=ve[b], du=du[b],
                    dinv=dinv[a], u=u[a], uinv=uinv[a], vinv=vinv[b], x=row_of(x, a), y=row_of(y, b),
                )
            )
        finish(ready, new_r, new_l)


def last_kernel(
    scal, cc, ff, pa, pd, pb, pe, ad_next, ad_prev, be_prev, be_next,
    er_own, er_came, el_own, el_one, el_two, el_three, r_own, r_came, l_own, l_one, l_two, l_three,
    r0, l0, r1, l1, r2, l2, c_out, f_out, r_out, l_out,
    c_buf, f_buf, a_buf, d_buf, b_buf, e_buf, r_buf, l_buf, zero, in_sem, own_sem, out_sem, tile_sem,
):
    role, shift, row, col = (scal[0], scal[1], scal[2], scal[3])
    copy = pltpu.make_async_copy
    held = ((cc, c_buf), (ff, f_buf), (pa, a_buf), (pd, d_buf), (pb, b_buf), (pe, e_buf))
    coming = {
        a: [copy(src.at[a], buf.at[a], in_sem.at[a, n]) for n, (src, buf) in enumerate(held)] for a in range(3)
    }
    for a in (2, 1, 0):
        for one in coming[a]:
            one.start()
    for at, (own_r, own_l) in enumerate(((r0, l0), (r1.at[1], l1.at[1]), (r2, l2))):

        @pl.when(role == at)
        def _(own_r=own_r, own_l=own_l):
            copy(own_r, r_buf, own_sem.at[0]).start()
            copy(own_l, l_buf, own_sem.at[1]).start()

    zero[...] = jnp.zeros_like(zero)
    have_er, have_el, have_r, have_l = [scal[4 + i] == 1 for i in range(4)]

    def front_r(s, b):
        if s == 2:
            return jnp.where(have_r, r_own[b], r_came[b])
        return jnp.where(have_er, er_own[s, b], er_came[s, b])

    def front_l(s, a):
        if s == 2:
            return jnp.where(have_l, l_own[a], l_one[a] + l_two[a] + l_three[a])
        return jnp.where(have_el, el_own[s, a], el_one[s, a] + el_two[s, a] + el_three[s, a])

    diff = col - row


    def tile(at, a, b):
        nxt = at + jnp.where(col == SIDE - 1, 1, 0) if b < 2 else at
        prv = at - jnp.where(col == 0, 1, 0) if b > a else at
        above = at - jnp.where(row == 0, 2 if a == 1 else 1, 0) if a > 0 else at
        below = at + jnp.where(row == SIDE - 1, 2 if a == 0 else 1, 0) if b > a else at
        tiles_c = (ad_next[0, nxt], a_buf[a, b], ad_prev[0, prv])
        tiles_f = (ad_next[1, nxt], d_buf[a, b], ad_prev[1, prv])
        lines_c = (be_prev[0, above], b_buf[a, b], be_next[0, below])
        lines_f = (be_prev[1, above], e_buf[a, b], be_next[1, below])
        parts_r, parts_l = ([], [])
        for s in range(3):
            on = SIDE * (b - a) + diff >= s
            parts_r.append(jnp.concatenate(split(jnp.where(on, front_r(s, b), 0.0)), axis=1))
            parts_l.append(jnp.concatenate(split(jnp.where(on, front_l(s, a), 0.0)), axis=0))
        across = jnp.concatenate([jnp.concatenate(tiles_c, axis=1), jnp.concatenate(tiles_f, axis=1)], axis=0)
        minus = dot(across, jnp.concatenate(parts_r, axis=0))
        down = jnp.concatenate([jnp.concatenate(lines_c, axis=0), jnp.concatenate(lines_f, axis=0)], axis=1)
        plus = dot(jnp.concatenate(parts_l, axis=1), down)
        minus = minus[:, :TILE] + minus[:, TILE:]
        plus = plus[:TILE] + plus[TILE:]
        c_buf[a, b] = c_buf[a, b] + (plus[:, :TILE] - minus[:TILE])
        f_buf[a, b] = f_buf[a, b] + (plus[:, TILE:] - minus[TILE:])

    sent = []
    for a in (2, 1, 0):
        for one in coming[a]:
            one.wait()
        for at, (i, b) in enumerate(UPPER):
            if i == a:
                tile(at, a, b)
        for n, (buf, out) in enumerate(((c_buf, c_out), (f_buf, f_out))):
            sent.append(copy(buf.at[a], out.at[a], out_sem.at[a, n]))
            sent[-1].start()
        if a == 2:

            @pl.when(role < 3)
            def _():
                copy(r0, r_buf, own_sem.at[0]).wait()
                copy(l0, l_buf, own_sem.at[1]).wait()

            for i in range(3):
                for b in range(3):
                    mine = (role < 3) & (i == b + shift)

                    @pl.when(mine)
                    def _(i=i, b=b):
                        copy(r_buf.at[b], r_out.at[i, b], tile_sem.at[i, b, 0]).start()
                        copy(l_buf.at[i], l_out.at[i, b], tile_sem.at[i, b, 1]).start()

                    @pl.when(jnp.logical_not(mine))
                    def _(i=i, b=b):
                        copy(zero, r_out.at[i, b], tile_sem.at[i, b, 0]).start()
                        copy(zero, l_out.at[i, b], tile_sem.at[i, b, 1]).start()

                    sent.append(copy(zero, r_out.at[i, b], tile_sem.at[i, b, 0]))
                    sent.append(copy(zero, l_out.at[i, b], tile_sem.at[i, b, 1]))
    for one in sent:
        one.wait()


def halves(*shape):
    return jax.ShapeDtypeStruct((*shape, TILE, TILE), jnp.bfloat16)


SMEM = pl.BlockSpec(memory_space=pltpu.SMEM)
VMEM = pl.BlockSpec(memory_space=pltpu.VMEM)
THREE = jax.ShapeDtypeStruct((3, TILE, TILE), jnp.float32)
PAIR = jax.ShapeDtypeStruct((2, 3, TILE, TILE), jnp.float32)
NINE = jax.ShapeDtypeStruct((3, 3, TILE, TILE), jnp.float32)


def call(kernel, outs, flops, *args, left=0, kinds=()):
    buffers = [pltpu.VMEM((3, TILE, TILE), kind) for kind in kinds]
    return pl.pallas_call(
        kernel,
        out_shape=outs,
        in_specs=[SMEM] + [pl.BlockSpec(memory_space=pl.ANY)] * left + [VMEM] * (len(args) - 1 - left),
        scratch_shapes=[*buffers, pltpu.SemaphoreType.DMA((len(kinds), 3))] if kinds else [],
        out_specs=[VMEM] * len(outs),
        cost_estimate=pl.CostEstimate(flops=flops, bytes_accessed=4_000_000, transcendentals=0),
    )(*args)


def call_last(*args):
    anywhere = pl.BlockSpec(memory_space=pl.ANY)
    wide = pltpu.VMEM((3, 3, TILE, TILE), jnp.float32)
    thin = pltpu.VMEM((3, 3, TILE, TILE), jnp.bfloat16)
    line = pltpu.VMEM((3, TILE, TILE), jnp.float32)
    dma = pltpu.SemaphoreType.DMA
    return pl.pallas_call(
        last_kernel,
        out_shape=[NINE] * 4,
        in_specs=[SMEM] + [anywhere] * 6 + [VMEM] * 16 + [anywhere] * 6,
        out_specs=[anywhere] * 4,
        scratch_shapes=[
            wide, wide, thin, thin, thin, thin, line, line, pltpu.VMEM((TILE, TILE), jnp.float32),
            dma((3, 6)), dma((2,)), dma((3, 2)), dma((3, 3, 2)),
        ],
        name="updates",
        cost_estimate=pl.CostEstimate(flops=1_500_000_000, bytes_accessed=8_000_000, transcendentals=0),
    )(*args)


def device(row, col):
    return (row % SIDE) * SIDE + col % SIDE


def send(value, pairs):
    return lax.ppermute(value, AXES, [(device(*s), device(*t)) for s, t in pairs])


class Tree:
    def __init__(self, value, roots):
        self.value, self.have, self.came, self.moves = (value, list(roots), [], ())

    def swap(self, move):
        self.came = [send(self.value, [((r, c), move(r, c)) for r in range(SIDE) for c in range(SIDE)])]

    def start(self, moves):
        self.moves = moves
        self.came = [send(self.value, [(s, move(*s)) for s in self.have]) for move in moves]
        self.have += [move(*s) for move in moves for s in self.have]

    def finish(self, own):
        self.value = jnp.where(own, self.value, functools.reduce(jnp.add, self.came))

    def after(self, other):
        self.value, _ = lax.optimization_barrier((self.value, other))

    def parts(self):
        return (self.value, *self.came)


def flip_row(bits):
    return lambda row, col: (row ^ bits, col)


def turn_row(step):
    return lambda row, col: ((row + step) % SIDE, col)


def turn_col(step):
    return lambda row, col: (row, (col + step) % SIDE)


def turn_low(step):
    return lambda row, col: (row, (col & ~3) | ((col + step) & 3))


ROW_LEVELS = ((flip_row(2),), (turn_row(4), turn_row(8), turn_row(12)), (flip_row(1),))
COL_LEVELS = ((turn_col(4), turn_col(8), turn_col(12)), (turn_low(1), turn_low(2), turn_low(3)))


def program(
    rhs_c, rhs_f, pencil_a, pencil_d, pencil_b, pencil_e, d_inverse, left_vectors, left_inverse,
    left_eigs, e_inverse, right_vectors, right_inverse, right_eigs,
):
    row = lax.axis_index("row").astype(jnp.int32)
    col = lax.axis_index("col").astype(jnp.int32)
    cc, ff, pa, pd, pb, pe = [
        v.transpose(0, 2, 1, 3) for v in (rhs_c, rhs_f, pencil_a, pencil_d, pencil_b, pencil_e)
    ]
    ahead = (col - row) % SIDE
    role = jnp.where(ahead == SIDE - 1, 0, jnp.where(ahead < 2, ahead + 1, 3))
    shift = jnp.where((role == 0) & (col == SIDE - 1), 1, jnp.where((role == 2) & (col == 0), -1, 0))
    odd = (row ^ col) & 1
    low = (row ^ col) & 3
    have_early_r = jnp.where(odd == 0, 1, 0)
    have_early_l = jnp.where(low == 0, 1, 0)
    have_late_r = jnp.where(odd == 1, 1, 0)
    have_late_l = jnp.where(((row + 1) ^ col) & 3 == 0, 1, 0)
    scal = jnp.stack([role, shift, row, col, have_early_r, have_early_l, have_late_r, have_late_l])
    ring = range(SIDE)
    left = (d_inverse, left_vectors, left_inverse, left_eigs)

    right = (e_inverse, right_vectors, right_inverse)

    a_own, e_own, near_ad, near_be = call(
        own_kernel, [halves(3), halves(3), halves(2, 3), halves(2, 3)], 1_000_000, scal, pa, pd, pb, pe
    )
    a_came = send(a_own, [((r, r), (r, r - 1)) for r in ring])
    e_came = send(e_own, [((c, c), (c + 1, c)) for c in ring])
    ad_near = send(near_ad, [((r, r + k), (r, r + k - 1)) for r in ring for k in (1, 2)])
    be_near = send(near_be, [((r, r + k), (r + 1, r + k)) for r in ring for k in (1, 2)])
    up = [(i, (i + 1) % SIDE) for i in ring]
    down = [(j, i) for i, j in up]

    ux, g, ve, du, r0, l0 = call(
        first_kernel, [THREE] * 6, 400_000_000,
        scal, cc, ff, a_own, e_own, a_came, e_came, *left, *right, right_eigs, left=2, kinds=(jnp.float32,) * 2,
    )
    r0_one = send(r0, [((c + 1, c), (c, c)) for c in ring])
    l0_one = send(l0, [((r, r - 1), (r, r)) for r in ring])
    a_late, e_late, _ = lax.optimization_barrier((a_own, e_own, r0))
    a_prev = send(a_late, [((r, r), (r, r + 1)) for r in ring])
    e_next = send(e_late, [((c, c), (c - 1, c)) for c in ring])
    made = call(
        ready_kernel, [THREE] * 4, 100_000_000,
        scal, a_prev, e_next, *left[:3], *right,
    )

    upper_ad, upper_be = call(
        upper_kernel, [halves(2, 6), halves(2, 6)], 20_000_000,
        lax.optimization_barrier((scal, r0))[0], pa, pd, pb, pe,
    )
    ad_next = lax.ppermute(upper_ad, "col", down)
    ad_prev = lax.ppermute(upper_ad, "col", up)
    tiles = (scal, cc, ff, pa, pd, pb, pe, ad_near, be_near)
    factors = (*left, right_inverse, right_eigs)
    r0_one = lax.optimization_barrier((r0_one, made[0]))[0]
    r1, l1 = call(
        functools.partial(next_kernel, 1), [PAIR] * 2, 400_000_000,
        *tiles, r0_one, l0_one, *factors, ux, g, ve, du, left=6, kinds=(jnp.float32,) * 2,
    )
    r_old = send(r1, [((c, c), (c - 1, c)) for c in ring])
    l_old = send(l1, [((r, r), (r, r + 1)) for r in ring])

    early_r = Tree(r1, [(c, c) for c in ring])
    early_l = Tree(l1, [(r, r) for r in ring])
    near = row ^ col
    early_l.start(COL_LEVELS[0])
    early_r.start(ROW_LEVELS[0])
    be_prev = lax.ppermute(lax.optimization_barrier((upper_be, r1))[0], "row", up)
    be_next = lax.ppermute(lax.optimization_barrier((upper_be, r1))[0], "row", down)
    r2, l2 = call(
        functools.partial(next_kernel, 2), [THREE] * 2, 400_000_000,
        *tiles, r_old, l_old, *factors, *made, left=6,
        kinds=(jnp.float32,) * 2 + (jnp.bfloat16,) * 4,
    )

    late_r = Tree(r2, [((c - 1) % SIDE, c) for c in ring])
    late_l = Tree(l2, [(r, (r + 1) % SIDE) for r in ring])
    far_r = row ^ ((col - 1) % SIDE)
    far_l = col ^ ((row + 1) % SIDE)
    late_r.start(ROW_LEVELS[0])
    late_l.start(COL_LEVELS[0])
    early_r.finish(near == 0)
    early_l.finish(near == 0)
    early_r.after(r2)
    early_l.after(r2)
    early_r.start(ROW_LEVELS[1])
    early_l.start(COL_LEVELS[1])
    late_r.finish(far_r == 0)
    late_l.finish(far_l == 0)
    late_r.start(ROW_LEVELS[1])
    late_l.start(COL_LEVELS[1])
    early_r.finish(near & ~2 == 0)
    early_r.swap(ROW_LEVELS[2][0])
    late_r.finish(far_r & ~2 == 0)
    late_r.swap(ROW_LEVELS[2][0])

    outs = call_last(
        scal, cc, ff, pa, pd, pb, pe, ad_next, ad_prev, be_prev, be_next,
        *early_r.parts(), *early_l.parts(), *late_r.parts(), *late_l.parts(), r0, l0, r1, l1, r2, l2,
    )
    return tuple(v.transpose(0, 2, 1, 3) for v in outs)


def solution(mesh):
    tile = P(None, "row", None, "col")
    lines = (P(None, "row", None),) * 3 + (P(None, "row"),)
    cols = (P(None, "col", None),) * 3 + (P(None, "col"),)
    return jax.shard_map(
        program, mesh=mesh, in_specs=(tile,) * 6 + lines + cols, out_specs=(tile,) * 4, check_vma=False
    )
```
